256 devices in a mesh: expert: 64 (over x, z, core), dp: 4 (over y).
Axes of the slice: x: 4, y: 4, z: 8, core: 2. Of those that a mesh axis runs over, the one named last changes fastest.
Arguments:
- tokens: bfloat16 [65536, 5120], P(('dp', 'expert')), parts along dimension 0, may hold values from -6 to 6
- router_logit: float32 [65536], P(('dp', 'expert')), parts along dimension 0, may hold values from 0 to 3
- expert_id: int32 [65536], P(('dp', 'expert')), parts along dimension 0, may hold values from 0 to 63, as said below
- token_slot: int32 [65536], P(('dp', 'expert')), parts along dimension 0, may hold values from 0 to 7, as said below
- keep: int32 [65536], P(('dp', 'expert')), parts along dimension 0, may hold values 0 or 1
- overflow_host: int32 [64, 4], replicated, may hold values from 0 to 63, as said below
- expert_gate: bfloat16 [64, 5120, 256], P('expert'), may hold values from -0.125 to 0.125
- expert_up: bfloat16 [64, 5120, 256], P('expert'), may hold values from -0.125 to 0.125
- expert_down: bfloat16 [64, 256, 5120], P('expert'), may hold values from -0.375 to 0.375
- shared_gate: bfloat16 [5120, 64], replicated, may hold values from -0.078125 to 0.078125
- shared_up: bfloat16 [5120, 64], replicated, may hold values from -0.078125 to 0.078125
- shared_down: bfloat16 [64, 5120], replicated, may hold values from -0.1875 to 0.1875
Outputs:
- moe_out: bfloat16 [65536, 5120], P(('dp', 'expert')), parts along dimension 0
The draws below stay inside these ranges and needn't reach their ends.
There are 4 independent parts, one for each index of `dp`. The reference program is written for one: setup_inputs(seed, part) draws one part's arguments, and reference() takes and returns one part's arrays. A program takes and returns all parts, laid end to end along the dimension named above; an argument that names none is the same for every part. Nothing has to cross between parts.
Inputs may be any that keep to these rules, and one draw needn't show every extreme that they name: `expert_id`: among the 256 tokens of one device at most 8 name the same expert; some experts are named by exactly 8 tokens of every device. `token_slot`: if c tokens of one device name the same expert, their slots are 0 to c - 1, each once. overflow_host[e, j] is e + 1 or e - 1, taken modulo 64.
All inputs are finite; a program needn't handle non-finite values. No bound on the sum of `keep` on one device may be relied on, other than what follows from the above.
Results may differ from the reference program's by a relative error of at most 0.007.
Values may be sent and summed in bfloat16 or wider, within the bound.
No kernel may reach another device: no remote copies, remote signals or barrier semaphores. Data moves between devices by JAX's collectives and lax.ppermute only.
A program may use at most 128 MiB of HBM per device.

```python
import jax
import jax.numpy as jnp
from jax import lax

D = 5120
F = 256
SH = 64
T_DEV = 256
EXPERTS = 64
TOKENS = 16384
SLOTS = 8
HOME = 4
SPILL = 4


def draw_tokens(key, part):
    base_key = jax.random.fold_in(key, 31)
    key_row, key_value = jax.random.split(base_key, 2)
    values = jnp.clip(jax.random.normal(key_value, (TOKENS, D), jnp.float32), -6.0, 6.0)
    return values.astype(jnp.bfloat16)


def routing_pair(key):
    base_key = jax.random.fold_in(key, 11)
    key_hot, key_score, key_order = jax.random.split(base_key, 3)
    devices = TOKENS // T_DEV
    cell_count = EXPERTS * SLOTS
    hot_count = max(1, EXPERTS // 8)
    hot_rank = jax.random.permutation(key_hot, EXPERTS)
    is_hot = (hot_rank < hot_count).astype(jnp.int32)
    cell_ids = jnp.arange(cell_count, dtype=jnp.int32)
    noise_bits = jax.random.randint(key_score, (devices, cell_count), 0, 1 << 16)
    cell_score = is_hot[cell_ids // SLOTS][None, :] * (1 << 28) + noise_bits * cell_count + cell_ids[None, :]
    unused, chosen = lax.top_k(cell_score, T_DEV)
    device_ids = jnp.arange(devices, dtype=jnp.int32)[:, None]
    picked = jnp.zeros((devices, cell_count), jnp.int32).at[device_ids, chosen].set(1)
    slot_rank = jnp.cumsum(picked.reshape(devices, EXPERTS, SLOTS), axis=2).reshape(devices, cell_count) - 1
    chosen_rank = jnp.take_along_axis(slot_rank, chosen, axis=1)
    order_keys = jax.random.randint(key_order, (devices, T_DEV), 0, 1 << 16) * T_DEV + jnp.arange(T_DEV, dtype=jnp.int32)[None, :]
    token_order = jnp.argsort(order_keys, axis=1)
    token_cell = jnp.take_along_axis(chosen, token_order, axis=1)
    token_slots = jnp.take_along_axis(chosen_rank, token_order, axis=1)
    return ((token_cell // SLOTS).reshape(-1).astype(jnp.int32), token_slots.reshape(-1).astype(jnp.int32))


def draw_expert_id(key, part):
    return routing_pair(key)[0]


def draw_token_slot(key, part):
    return routing_pair(key)[1]


def draw_overflow_host(key, part):
    side_bits = jax.random.randint(jax.random.fold_in(key, 23), (EXPERTS, SPILL), 0, 2)
    expert_ids = jnp.arange(EXPERTS, dtype=jnp.int32)[:, None]
    return ((expert_ids + 2 * side_bits - 1 + EXPERTS) % EXPERTS).astype(jnp.int32)


def with_ends(values, stream_key, least, largest):
    longest = values.shape.index(max(values.shape))
    spots = []
    for shift in (0, 1):
        where = [jax.random.randint(jax.random.fold_in(stream_key, axis), (), 0, length) for axis, length in enumerate(values.shape)]
        where[longest] = (where[longest] + shift) % values.shape[longest]
        spots.append(tuple(where))
    return values.at[spots[0]].set(least).at[spots[1]].set(largest)


def level_of(own_key, dims, shards, least, top_value):
    gain, own = 1.0, jax.random.fold_in(own_key, 6)
    for dim, parts in shards:
        draws = jnp.exp(jax.random.uniform(jax.random.fold_in(own, dim), (parts,), jnp.float32, least / len(shards), top_value / len(shards)))
        gain = gain * jnp.repeat(draws, dims[dim] // parts).reshape([-1 if axis == dim else 1 for axis in range(len(dims))])
    return gain


def normal_values(own_key, shape, width, reach, shards=(), kind=jnp.bfloat16):
    gain = level_of(own_key, shape, shards, -0.22, 0.18) if shards else 1.0
    entries = jax.random.normal(own_key, shape, jnp.float32) * width * gain
    return jnp.minimum(jnp.maximum(entries, -reach), reach).astype(kind)


def setup_inputs(seed: int = 0, part: int = 0) -> dict:
    key_list = jax.random.split(jax.random.key(seed), 13)
    part_splits = jax.random.split(jax.random.fold_in(key_list[12], part), 13)
    return {
        "tokens": draw_tokens(jax.random.fold_in(jax.random.fold_in(key_list[12], part), 71), part),
        "router_logit": jnp.clip(3.0 * jax.random.uniform(part_splits[1], (TOKENS,), jnp.float32) ** level_of(part_splits[1], (TOKENS,), ((0, 64),), -0.2, 0.2), 0.0, 3.0),
        "expert_id": draw_expert_id(jax.random.fold_in(jax.random.fold_in(key_list[12], part), 71), part),
        "token_slot": draw_token_slot(jax.random.fold_in(jax.random.fold_in(key_list[12], part), 71), part),
        "keep": with_ends((jax.random.randint(part_splits[4], (TOKENS,), 0, 8) < 7).astype(jnp.int32), jax.random.fold_in(part_splits[4], 1), 0, 1),
        "overflow_host": draw_overflow_host(jax.random.fold_in(key_list[12], 71), part),
        "expert_gate": normal_values(key_list[6], (EXPERTS, D, F), (D // 2) ** -0.5, 0.125, ((0, 64),)),
        "expert_up": normal_values(key_list[7], (EXPERTS, D, F), (D // 2) ** -0.5, 0.125, ((0, 64),)),
        "expert_down": normal_values(key_list[8], (EXPERTS, F, D), F ** -0.5, 0.375, ((0, 64),)),
        "shared_gate": normal_values(key_list[9], (D, SH), D ** -0.5, 0.078125),
        "shared_up": normal_values(key_list[10], (D, SH), D ** -0.5, 0.078125),
        "shared_down": normal_values(key_list[11], (SH, D), (16 * SH) ** -0.5, 0.1875),
    }


def reference(tokens, router_logit, expert_id, token_slot, keep, overflow_host, expert_gate, expert_up, expert_down, shared_gate, shared_up, shared_down):
    token_scale = jax.nn.sigmoid(router_logit) * keep.astype(jnp.float32)
    routed_in = (tokens.astype(jnp.float32) * token_scale[:, None]).astype(jnp.bfloat16)
    is_spill = token_slot >= HOME
    spill_level = jnp.maximum(token_slot - HOME, 0).astype(jnp.int32)
    host_expert = overflow_host[expert_id, spill_level].astype(jnp.int32)
    served = jnp.where(is_spill, host_expert, expert_id).astype(jnp.int32)
    lane_count = HOME + 2 * SPILL
    positions = jnp.arange(TOKENS, dtype=jnp.int32)
    source_device = positions // T_DEV
    to_right = host_expert == (expert_id + 1) % EXPERTS
    lane_index = jnp.where(is_spill, jnp.where(to_right, HOME + spill_level, HOME + SPILL + spill_level), token_slot)
    column_index = (source_device * lane_count + lane_index).astype(jnp.int32)
    token_table = jnp.full((EXPERTS, EXPERTS * lane_count), TOKENS, jnp.int32).at[served, column_index].set(positions)
    padded = jnp.concatenate([routed_in, jnp.zeros((1, D), jnp.bfloat16)], axis=0)

    def one_expert(partial_value, inputs):
        index_row, w_gate, w_up, w_down = inputs
        chosen = padded[index_row]
        gate_out = jnp.dot(chosen, w_gate, preferred_element_type=jnp.float32)
        up_out = jnp.dot(chosen, w_up, preferred_element_type=jnp.float32)
        hidden = (jax.nn.silu(gate_out) * up_out).astype(jnp.bfloat16)
        result = jnp.dot(hidden, w_down, preferred_element_type=jnp.float32).astype(jnp.bfloat16)
        return partial_value.at[index_row].set(result), None

    routed, unused = lax.scan(one_expert, jnp.zeros((TOKENS + 1, D), jnp.bfloat16), (token_table, expert_gate, expert_up, expert_down))
    shared_hidden = (jax.nn.silu(jnp.dot(tokens, shared_gate, preferred_element_type=jnp.float32)) * jnp.dot(tokens, shared_up, preferred_element_type=jnp.float32)).astype(jnp.bfloat16)
    shared_out = jnp.dot(shared_hidden, shared_down, preferred_element_type=jnp.float32)
    return (shared_out + routed[:TOKENS].astype(jnp.float32)).astype(jnp.bfloat16)
```

```python
import functools

import jax
import jax.numpy as jnp
from jax import lax
from jax.experimental import pallas as pl
from jax.experimental.pallas import tpu as pltpu
from jax.sharding import PartitionSpec as P


LANES = 128
F32 = jnp.float32
BF16 = jnp.bfloat16


def dot(a, b):
    return jnp.dot(a, b, preferred_element_type=F32)


def cost(flops, nbytes):
    return pl.CostEstimate(flops=flops, bytes_accessed=nbytes, transcendentals=0)


def params():
    return pltpu.CompilerParams(dimension_semantics=("arbitrary",))


def route_kernel(logit_ref, id_ref, slot_ref, keep_ref, tok_ref, out_ref, *, slots):
    rows = out_ref.shape[0]
    cell = id_ref[...] * slots + slot_ref[...]
    scale = jax.nn.sigmoid(logit_ref[...]) * keep_ref[...].astype(F32)
    hit = lax.broadcasted_iota(jnp.int32, (rows, cell.shape[1]), 0) == cell
    row_scale = jnp.sum(jnp.where(hit, scale, 0.0), axis=1, keepdims=True)
    picked = dot(hit.astype(F32).astype(BF16), tok_ref[...])
    out_ref[...] = (picked * row_scale).astype(BF16)


def route(logit, ids, slot, keep, tokens, rows, slots, block):
    count, width = tokens.shape
    small = pl.BlockSpec((1, count), lambda j: (0, 0))
    return pl.pallas_call(
        functools.partial(route_kernel, slots=slots),
        grid=(width // block,),
        in_specs=[small, small, small, small, pl.BlockSpec((count, block), lambda j: (0, j))],
        out_specs=pl.BlockSpec((rows, block), lambda j: (0, j)),
        out_shape=jax.ShapeDtypeStruct((rows, width), BF16),
        compiler_params=params(),
        cost_estimate=cost(2 * rows * count * width, 2 * width * (rows + count)),
        name="route",
    )(logit, ids, slot, keep, tokens)


def pack_kernel(order_ref, g_ref, u_ref, d_ref, out_ref):
    out_ref[0] = g_ref[...]
    out_ref[1] = u_ref[...]
    out_ref[2] = d_ref[...]


def pack(order, gate, up_, down_, planes):
    model, hidden = gate.shape
    steps = model // planes // hidden
    tall = pl.BlockSpec((hidden, hidden), lambda i, o: (o[0] * steps + i, 0))
    flat = pl.BlockSpec((hidden, hidden), lambda i, o: (0, o[0] * steps + i))
    out = pl.pallas_call(
        pack_kernel,
        grid_spec=pltpu.PrefetchScalarGridSpec(
            num_scalar_prefetch=1,
            grid=(steps,),
            in_specs=[tall, tall, flat],
            out_specs=pl.BlockSpec((3, hidden, hidden), lambda i, o: (0, i, 0)),
        ),
        out_shape=jax.ShapeDtypeStruct((3, model // planes, hidden), BF16),
        compiler_params=params(),
        name="pack",
    )(order, gate, up_, down_)
    return out.reshape(3 * model // planes, hidden)


def up_kernel(flag_ref, order_ref, x_ref, g0, u0, g1, u1, g2, u2, out_ref, wide, acc, *, sources, slots):
    step = pl.program_id(0)
    half = slots // 2
    rows = sources * half

    @pl.when(step == 0)
    def _():
        acc[...] = jnp.zeros_like(acc)

    tall, tiles = x_ref.shape[0], x_ref.shape[1] // LANES
    for c in range(tiles):
        wide[c * tall : (c + 1) * tall, :] = x_ref[:, c * LANES : (c + 1) * LANES].astype(F32)
    parts = [
        jnp.concatenate(
            [wide[pl.ds(c * tall + s, sources, stride=slots), :].astype(BF16) for c in range(tiles)], axis=1
        )
        for s in range(slots)
    ]
    home = jnp.concatenate(parts[:half], axis=0)
    hidden = g0.shape[-1]
    acc[0:rows, 0:hidden] += dot(home, g0[...])
    acc[0:rows, hidden:] += dot(home, u0[...])
    for j in range(half):
        x = parts[half + j]
        lo = rows + j * sources

        @pl.when(flag_ref[j] == 1)
        def _():
            acc[lo : lo + sources, 0:hidden] += dot(x, g1[...])
            acc[lo : lo + sources, hidden:] += dot(x, u1[...])

        @pl.when(flag_ref[j] == 0)
        def _():
            acc[lo : lo + sources, 0:hidden] += dot(x, g2[...])
            acc[lo : lo + sources, hidden:] += dot(x, u2[...])

    @pl.when(step == pl.num_programs(0) - 1)
    def _():
        gate = acc[:, 0:hidden]
        out_ref[...] = (gate / (1.0 + jnp.exp(-gate)) * acc[:, hidden:]).astype(BF16)


def up(flags, order, x, own, partner, side, sources, slots, planes):
    rows, width = x.shape
    hidden = own[0].shape[-1]
    cuts = 2
    block = width // planes // cuts
    wspec = pl.BlockSpec((block, hidden), lambda k, f, o: (o[k // cuts] * cuts + k % cuts, 0))
    side_gate = pl.BlockSpec((None, block, hidden), lambda k, f, o: (k // cuts, k % cuts, 0))
    side_up = pl.BlockSpec((None, block, hidden), lambda k, f, o: (k // cuts, cuts + k % cuts, 0))
    return pl.pallas_call(
        functools.partial(up_kernel, sources=sources, slots=slots),
        grid_spec=pltpu.PrefetchScalarGridSpec(
            num_scalar_prefetch=2,
            grid=(planes * cuts,),
            in_specs=[pl.BlockSpec((rows, block), lambda k, f, o: (0, o[k // cuts] * cuts + k % cuts))]
            + [wspec] * 4
            + [side_gate, side_up],
            out_specs=pl.BlockSpec((rows, hidden), lambda k, f, o: (0, 0)),
            scratch_shapes=[pltpu.VMEM((rows * block // LANES, LANES), F32), pltpu.VMEM((rows, 2 * hidden), F32)],
        ),
        out_shape=jax.ShapeDtypeStruct((rows, hidden), BF16),
        compiler_params=params(),
        cost_estimate=cost(4 * rows * width * hidden, 2 * width * (rows + 6 * hidden)),
        name="up",
    )(flags, order, x, own[0], own[1], partner[0], partner[1], side, side)


def down_kernel(flag_ref, order_ref, h_ref, d0, d1, d2, out_ref, wide, *, sources, slots):
    half = slots // 2
    rows = sources * half
    tall, tiles = out_ref.shape[0], out_ref.shape[1] // LANES

    def place(slot, block):
        for c in range(tiles):
            wide[pl.ds(c * tall + slot, sources, stride=slots), :] = block[:, c * LANES : (c + 1) * LANES]

    home = dot(h_ref[0:rows, :], d0[...])
    for s in range(half):
        place(s, home[s * sources : (s + 1) * sources, :])
    for j in range(half):
        h = h_ref[rows + j * sources : rows + (j + 1) * sources, :]

        @pl.when(flag_ref[j] == 1)
        def _():
            place(half + j, dot(h, d1[...]))

        @pl.when(flag_ref[j] == 0)
        def _():
            hidden = d2.shape[1]
            cuts = [dot(h, d2[i * hidden : (i + 1) * hidden, :]) for i in range(d2.shape[0] // hidden)]
            place(half + j, jnp.concatenate(cuts, axis=1))

    for c in range(tiles):
        out_ref[:, c * LANES : (c + 1) * LANES] = wide[c * tall : (c + 1) * tall, :].astype(BF16)


def down(flags, order, h, own, partner, side, sources, slots, planes):
    rows, hidden = h.shape
    width = own.shape[1]
    block = width // planes
    wspec = pl.BlockSpec((hidden, block), lambda j, f, o: (0, o[j]))
    return pl.pallas_call(
        functools.partial(down_kernel, sources=sources, slots=slots),
        grid_spec=pltpu.PrefetchScalarGridSpec(
            num_scalar_prefetch=2,
            grid=(planes,),
            in_specs=[
                pl.BlockSpec((rows, hidden), lambda j, f, o: (0, 0)),
                wspec,
                wspec,
                pl.BlockSpec((None, block, hidden), lambda j, f, o: (j, 2, 0)),
            ],
            out_specs=pl.BlockSpec((rows, block), lambda j, f, o: (0, o[j])),
            scratch_shapes=[pltpu.VMEM((rows * block // LANES, LANES), F32)],
        ),
        out_shape=jax.ShapeDtypeStruct((rows, width), BF16),
        compiler_params=params(),
        cost_estimate=cost(2 * rows * width * hidden, 2 * width * (rows + 3 * hidden)),
        name="down",
    )(flags, order, h, own, partner, side)


def finish_kernel(cell_ref, sh_ref, sd_ref, ans_ref, out_ref):
    count = cell_ref.shape[0]
    rows = ans_ref.shape[0]
    hit = lax.broadcasted_iota(jnp.int32, (count, rows), 1) == cell_ref[...]
    out = dot(hit.astype(F32).astype(BF16), ans_ref[...]) + dot(sh_ref[...], sd_ref[...])
    out_ref[...] = out.astype(BF16)


def finish(cell, sh, sd, answers, block):
    count = cell.shape[0]
    rows, width = answers.shape
    return pl.pallas_call(
        finish_kernel,
        grid=(width // block,),
        in_specs=[
            pl.BlockSpec((count, 1), lambda j: (0, 0)),
            pl.BlockSpec(sh.shape, lambda j: (0, 0)),
            pl.BlockSpec((sd.shape[0], block), lambda j: (0, j)),
            pl.BlockSpec((rows, block), lambda j: (0, j)),
        ],
        out_specs=pl.BlockSpec((count, block), lambda j: (0, j)),
        out_shape=jax.ShapeDtypeStruct((count, width), BF16),
        compiler_params=params(),
        cost_estimate=cost(2 * rows * count * width, 2 * width * (rows + 2 * count)),
        name="finish",
    )(cell, sh, sd, answers)


def exchange(x, experts):
    rows, width = x.shape
    x = x.reshape(experts, rows // experts, width)
    x = lax.all_to_all(x, "expert", split_axis=0, concat_axis=0, tiled=True)
    return x.reshape(rows, width)


def share(piece, planes):
    ahead = [(p, (p + 1) % planes) for p in range(planes)]
    back = [(p, (p - 1) % planes) for p in range(planes)]
    low = lax.ppermute(piece, "dp", ahead)
    high = lax.ppermute(piece, "dp", back)
    half = piece.shape[0] // 2
    far = jnp.concatenate([lax.ppermute(low[:half], "dp", ahead), lax.ppermute(high[half:], "dp", back)], axis=0)
    return jnp.stack([piece, low, high, far])


def body(
    tokens,
    router_logit,
    expert_id,
    token_slot,
    keep,
    overflow_host,
    expert_gate,
    expert_up,
    expert_down,
    shared_gate,
    shared_up,
    shared_down,
):
    experts = lax.axis_size("expert")
    planes = lax.axis_size("dp")
    myself = lax.axis_index("expert")
    count, model = tokens.shape
    slots = 2 * count // experts
    rows = experts * slots
    block = model // planes
    gate, up_, down_ = expert_gate[0], expert_up[0], expert_down[0]
    plane = lax.axis_index("dp")
    order = (plane + jnp.array([0, planes - 1, 1, 2], jnp.int32)) % planes
    side_pairs = [(e, (e + 1 if e % 2 else e - 1) % experts) for e in range(experts)]
    piece = lax.ppermute(pack(order, gate, up_, down_, planes), "expert", side_pairs)

    line = lambda v: v.reshape(1, count)
    routing = (line(router_logit), line(expert_id), line(token_slot), line(keep))
    arrived = exchange(route(*routing, tokens, rows, slots, block), experts)

    side = share(piece, planes)
    partner_pairs = [(e, e ^ 1) for e in range(experts)]
    gate1, up1, down1 = [lax.ppermute(w, "expert", partner_pairs) for w in (gate, up_, down_)]
    host_row = lax.dynamic_index_in_dim(overflow_host, myself, 0, keepdims=False)
    flags = (host_row == (myself ^ 1)).astype(jnp.int32)

    hidden = up(flags, order, arrived, (gate, up_), (gate1, up1), side, experts, slots, planes)
    reply = down(flags, order, hidden, down_, down1, side, experts, slots, planes)
    answers = exchange(reply, experts)
    shared_hidden = (
        jax.nn.silu(jnp.dot(tokens, shared_gate, preferred_element_type=F32))
        * jnp.dot(tokens, shared_up, preferred_element_type=F32)
    ).astype(BF16)
    cell = (expert_id * slots + token_slot).reshape(count, 1)
    return finish(cell, shared_hidden, shared_down, answers, block)


def solution(mesh):
    return jax.shard_map(
        body,
        mesh=mesh,
        in_specs=(
            P(("dp", "expert"), None),
            P(("dp", "expert")),
            P(("dp", "expert")),
            P(("dp", "expert")),
            P(("dp", "expert")),
            P(),
            P("expert", None, None),
            P("expert", None, None),
            P("expert", None, None),
            P(),
            P(),
            P(),
        ),
        out_specs=P(("dp", "expert"), None),
        check_vma=False,
    )
```

```python
import functools

import jax
import jax.numpy as jnp
from jax import lax
from jax.experimental import pallas as pl
from jax.experimental.pallas import tpu as pltpu
from jax.sharding import PartitionSpec as P


LANES = 128
F32 = jnp.float32
BF16 = jnp.bfloat16


def dot(a, b):
    return jnp.dot(a, b, preferred_element_type=F32)


def cost(flops, nbytes):
    return pl.CostEstimate(flops=flops, bytes_accessed=nbytes, transcendentals=0)


def params():
    return pltpu.CompilerParams(dimension_semantics=("arbitrary",))


def route_kernel(logit_ref, id_ref, slot_ref, keep_ref, tok_ref, out_ref, *, slots):
    rows = out_ref.shape[0]
    cell = id_ref[...] * slots + slot_ref[...]
    scale = jax.nn.sigmoid(logit_ref[...]) * keep_ref[...].astype(F32)
    hit = lax.broadcasted_iota(jnp.int32, (rows, cell.shape[1]), 0) == cell
    row_scale = jnp.sum(jnp.where(hit, scale, 0.0), axis=1, keepdims=True)
    picked = dot(hit.astype(F32).astype(BF16), tok_ref[...])
    out_ref[...] = (picked * row_scale).astype(BF16)


def route(logit, ids, slot, keep, tokens, rows, slots, block):
    count, width = tokens.shape
    small = pl.BlockSpec((1, count), lambda j: (0, 0))
    return pl.pallas_call(
        functools.partial(route_kernel, slots=slots),
        grid=(width // block,),
        in_specs=[small, small, small, small, pl.BlockSpec((count, block), lambda j: (0, j))],
        out_specs=pl.BlockSpec((rows, block), lambda j: (0, j)),
        out_shape=jax.ShapeDtypeStruct((rows, width), BF16),
        compiler_params=params(),
        cost_estimate=cost(2 * rows * count * width, 2 * width * (rows + count)),
        name="route",
    )(logit, ids, slot, keep, tokens)


def pack_kernel(order_ref, g_ref, u_ref, d_ref, out_ref):
    out_ref[0] = g_ref[...]
    out_ref[1] = u_ref[...]
    out_ref[2] = d_ref[...]


def pack(order, gate, up_, down_, planes):
    model, hidden = gate.shape
    steps = model // planes // hidden
    tall = pl.BlockSpec((hidden, hidden), lambda i, o: (o[0] * steps + i, 0))
    flat = pl.BlockSpec((hidden, hidden), lambda i, o: (0, o[0] * steps + i))
    out = pl.pallas_call(
        pack_kernel,
        grid_spec=pltpu.PrefetchScalarGridSpec(
            num_scalar_prefetch=1,
            grid=(steps,),
            in_specs=[tall, tall, flat],
            out_specs=pl.BlockSpec((3, hidden, hidden), lambda i, o: (0, i, 0)),
        ),
        out_shape=jax.ShapeDtypeStruct((3, model // planes, hidden), BF16),
        compiler_params=params(),
        name="pack",
    )(order, gate, up_, down_)
    return out.reshape(3 * model // planes, hidden)


def ffn_kernel(
    flag_ref, order_ref, x_ref, g0, u0, g1, u1, g2, u2, d0, d1, d2, out_ref, wide, home_acc, near_acc, far_acc, hid, *, sources, slots, up_steps
):
    step = pl.program_id(0)
    half = slots // 2
    rows = sources * half
    tall = sources * slots
    hidden = g0.shape[-1]

    @pl.when(step == 0)
    def _():
        home_acc[...] = jnp.zeros_like(home_acc)
        near_acc[...] = jnp.zeros_like(near_acc)
        far_acc[...] = jnp.zeros_like(far_acc)

    @pl.when(step < up_steps)
    def _():
        tiles = x_ref.shape[1] // LANES
        for c in range(tiles):
            wide[c * tall : (c + 1) * tall, :] = x_ref[:, c * LANES : (c + 1) * LANES].astype(F32)

        def group(first):
            return jnp.concatenate(
                [
                    jnp.concatenate(
                        [wide[pl.ds(c * tall + s, sources, stride=slots), :].astype(BF16) for s in range(first, first + half)],
                        axis=0,
                    )
                    for c in range(tiles)
                ],
                axis=1,
            )

        home, spill = group(0), group(half)
        home_acc[:, 0:hidden] += dot(home, g0[...])
        home_acc[:, hidden:] += dot(home, u0[...])
        near_acc[:, 0:hidden] += dot(spill, g1[...])
        near_acc[:, hidden:] += dot(spill, u1[...])
        far_acc[:, 0:hidden] += dot(spill, g2[...])
        far_acc[:, hidden:] += dot(spill, u2[...])

    def activate(acc):
        gate = acc[:, 0:hidden]
        return (gate / (1.0 + jnp.exp(-gate)) * acc[:, hidden:]).astype(BF16)

    @pl.when(step == up_steps - 1)
    def _():
        hid[0:rows, :] = activate(home_acc[...])
        for j in range(half):
            cut = slice(j * sources, (j + 1) * sources)
            use_near = flag_ref[j] == 1
            mine = activate(jnp.where(use_near, near_acc[cut, :], far_acc[cut, :])).astype(F32)
            hid[rows + cut.start : rows + cut.stop, :] = jnp.where(use_near, mine, 0.0).astype(BF16)
            hid[2 * rows + cut.start : 2 * rows + cut.stop, :] = jnp.where(use_near, 0.0, mine).astype(BF16)

    @pl.when(step >= up_steps)
    def _():
        tiles = out_ref.shape[1] // LANES
        home = dot(hid[0:rows, :], d0[...])
        far = jnp.concatenate(
            [dot(hid[2 * rows :, :], d2[i * hidden : (i + 1) * hidden, :]) for i in range(d2.shape[0] // hidden)], axis=1
        )
        spill = dot(hid[rows : 2 * rows, :], d1[...]) + far
        for c in range(tiles):
            lanes = slice(c * LANES, (c + 1) * LANES)
            for s in range(half):
                cut = slice(s * sources, (s + 1) * sources)
                wide[pl.ds(c * tall + s, sources, stride=slots), :] = home[cut, lanes]
                wide[pl.ds(c * tall + half + s, sources, stride=slots), :] = spill[cut, lanes]
            out_ref[:, lanes] = wide[c * tall : (c + 1) * tall, :].astype(BF16)


def ffn(flags, order, x, own, partner, side, sources, slots, planes, cuts=1):
    rows, width = x.shape
    hidden = own[0].shape[-1]
    wide = width // planes
    block = wide // cuts
    up_steps = planes * cuts

    def piece(k):
        return jnp.minimum(k // cuts, planes - 1)

    def cut(k):
        return jnp.where(k < up_steps, k % cuts, cuts - 1)

    def late(k):
        return jnp.maximum(k - up_steps, 0)

    col = lambda k, o: o[piece(k)] * cuts + cut(k)
    tall = pl.BlockSpec((block, hidden), lambda k, f, o: (col(k, o), 0))
    side_gate = pl.BlockSpec((None, block, hidden), lambda k, f, o: (piece(k), cut(k), 0))
    side_up = pl.BlockSpec((None, block, hidden), lambda k, f, o: (piece(k), cuts + cut(k), 0))
    flat = pl.BlockSpec((hidden, wide), lambda k, f, o: (0, o[late(k)]))
    side_down = pl.BlockSpec((None, wide, hidden), lambda k, f, o: (late(k), 2, 0))
    half = rows // 2
    return pl.pallas_call(
        functools.partial(ffn_kernel, sources=sources, slots=slots, up_steps=up_steps),
        grid_spec=pltpu.PrefetchScalarGridSpec(
            num_scalar_prefetch=2,
            grid=(up_steps + planes,),
            in_specs=[
                pl.BlockSpec((rows, block), lambda k, f, o: (0, col(k, o))),
                tall,
                tall,
                tall,
                tall,
                side_gate,
                side_up,
                flat,
                flat,
                side_down,
            ],
            out_specs=pl.BlockSpec((rows, wide), lambda k, f, o: (0, o[late(k)])),
            scratch_shapes=[pltpu.VMEM((rows * wide // LANES, LANES), F32)]
            + [pltpu.VMEM((half, 2 * hidden), F32)] * 3
            + [pltpu.VMEM((3 * half, hidden), BF16)],
        ),
        out_shape=jax.ShapeDtypeStruct((rows, width), BF16),
        compiler_params=params(),
        cost_estimate=cost(6 * rows * width * hidden, 4 * width * (rows + 5 * hidden)),
        name="ffn",
    )(flags, order, x, own[0], own[1], partner[0], partner[1], side, side, own[2], partner[2], side)


def finish_kernel(cell_ref, sh_ref, sd_ref, ans_ref, out_ref):
    count = cell_ref.shape[0]
    rows = ans_ref.shape[0]
    hit = lax.broadcasted_iota(jnp.int32, (count, rows), 1) == cell_ref[...]
    out = dot(hit.astype(F32).astype(BF16), ans_ref[...]) + dot(sh_ref[...], sd_ref[...])
    out_ref[...] = out.astype(BF16)


def finish(cell, sh, sd, answers, block):
    count = cell.shape[0]
    rows, width = answers.shape
    return pl.pallas_call(
        finish_kernel,
        grid=(width // block,),
        in_specs=[
            pl.BlockSpec((count, 1), lambda j: (0, 0)),
            pl.BlockSpec(sh.shape, lambda j: (0, 0)),
            pl.BlockSpec((sd.shape[0], block), lambda j: (0, j)),
            pl.BlockSpec((rows, block), lambda j: (0, j)),
        ],
        out_specs=pl.BlockSpec((count, block), lambda j: (0, j)),
        out_shape=jax.ShapeDtypeStruct((count, width), BF16),
        compiler_params=params(),
        cost_estimate=cost(2 * rows * count * width, 2 * width * (rows + 2 * count)),
        name="finish",
    )(cell, sh, sd, answers)


def exchange(x, experts):
    rows, width = x.shape
    x = x.reshape(experts, rows // experts, width)
    x = lax.all_to_all(x, "expert", split_axis=0, concat_axis=0, tiled=True)
    return x.reshape(rows, width)


def share(piece, planes):
    ahead = [(p, (p + 1) % planes) for p in range(planes)]
    back = [(p, (p - 1) % planes) for p in range(planes)]
    low = lax.ppermute(piece, "dp", ahead)
    high = lax.ppermute(piece, "dp", back)
    half = piece.shape[0] // 2
    far = jnp.concatenate([lax.ppermute(low[:half], "dp", ahead), lax.ppermute(high[half:], "dp", back)], axis=0)
    return jnp.stack([piece, low, high, far])


def body(
    tokens,
    router_logit,
    expert_id,
    token_slot,
    keep,
    overflow_host,
    expert_gate,
    expert_up,
    expert_down,
    shared_gate,
    shared_up,
    shared_down,
):
    experts = lax.axis_size("expert")
    planes = lax.axis_size("dp")
    myself = lax.axis_index("expert")
    count, model = tokens.shape
    slots = 2 * count // experts
    rows = experts * slots
    block = model // planes
    gate, up_, down_ = expert_gate[0], expert_up[0], expert_down[0]
    plane = lax.axis_index("dp")
    order = (plane + jnp.array([0, planes - 1, 1, 2], jnp.int32)) % planes
    side_pairs = [(e, (e + 1 if e % 2 else e - 1) % experts) for e in range(experts)]
    packed = pack(order, gate, up_, down_, planes)
    piece = lax.ppermute(packed, "expert", side_pairs)

    line = lambda v: v.reshape(1, count)
    routing = (line(router_logit), line(expert_id), line(token_slot), line(keep))
    outgoing = route(*routing, tokens, rows, slots, 2 * block)
    arrived = exchange(outgoing, experts)

    side = share(piece, planes)
    partner_pairs = [(e, e ^ 1) for e in range(experts)]
    gate1, up1, down1 = [lax.ppermute(w, "expert", partner_pairs) for w in (gate, up_, down_)]
    host_row = lax.dynamic_index_in_dim(overflow_host, myself, 0, keepdims=False)
    flags = (host_row == (myself ^ 1)).astype(jnp.int32)

    reply = ffn(flags, order, arrived, (gate, up_, down_), (gate1, up1, down1), side, experts, slots, planes)
    answers = exchange(reply, experts)
    shared_hidden = (
        jax.nn.silu(jnp.dot(tokens, shared_gate, preferred_element_type=F32))
        * jnp.dot(tokens, shared_up, preferred_element_type=F32)
    ).astype(BF16)
    cell = (expert_id * slots + token_slot).reshape(count, 1)
    return finish(cell, shared_hidden, shared_down, answers, 2 * block)


def solution(mesh):
    return jax.shard_map(
        body,
        mesh=mesh,
        in_specs=(
            P(("dp", "expert"), None),
            P(("dp", "expert")),
            P(("dp", "expert")),
            P(("dp", "expert")),
            P(("dp", "expert")),
            P(),
            P("expert", None, None),
            P("expert", None, None),
            P("expert", None, None),
            P(),
            P(),
            P(),
        ),
        out_specs=P(("dp", "expert"), None),
        check_vma=False,
    )
```

```python
import functools

import jax
import jax.numpy as jnp
from jax import lax
from jax.experimental import pallas as pl
from jax.experimental.pallas import tpu as pltpu
from jax.sharding import PartitionSpec as P


LANES = 128
AHEAD = 3
CUTS = 2
F32 = jnp.float32
BF16 = jnp.bfloat16


def dot(a, b):
    return jnp.dot(a, b, preferred_element_type=F32)


def cost(flops, nbytes):
    return pl.CostEstimate(flops=flops, bytes_accessed=nbytes, transcendentals=0)


ANY = pl.BlockSpec(memory_space=pl.ANY)


def columns(ref, start, width):
    return ref.at[:, pl.ds(pl.multiple_of(start, LANES), width)]


def call(kernel, shape, specs, scratch, flops, nbytes):
    return pl.pallas_call(
        kernel,
        in_specs=specs,
        out_specs=ANY,
        out_shape=jax.ShapeDtypeStruct(shape, BF16),
        scratch_shapes=scratch,
        cost_estimate=cost(flops, nbytes),
    )


SCALARS = pl.BlockSpec(memory_space=pltpu.SMEM)


def route_kernel(order_ref, logit_ref, id_ref, slot_ref, keep_ref, tok_ref, out_ref, chosen, row_scale, *, slots):
    @pl.when(pl.program_id(0) == 0)
    def _():
        cell = id_ref[...] * slots + slot_ref[...]
        scale = jax.nn.sigmoid(logit_ref[...]) * keep_ref[...].astype(F32)
        hit = lax.broadcasted_iota(jnp.int32, chosen.shape, 0) == cell
        row_scale[...] = jnp.sum(jnp.where(hit, scale, 0.0), axis=1, keepdims=True)
        chosen[...] = hit.astype(F32).astype(BF16)

    out_ref[...] = (dot(chosen[...], tok_ref[...]) * row_scale[...]).astype(BF16)


def route(order, logit, ids, slot, keep, tokens, rows, slots, block, first, last):
    count = tokens.shape[0]
    small = pl.BlockSpec((1, count), lambda j, o: (0, 0))
    return pl.pallas_call(
        functools.partial(route_kernel, slots=slots),
        grid_spec=pltpu.PrefetchScalarGridSpec(
            num_scalar_prefetch=1,
            grid=(last - first,),
            in_specs=[small, small, small, small, pl.BlockSpec((count, block), lambda j, o: (0, o[first + j]))],
            out_specs=pl.BlockSpec((rows, block), lambda j, o: (0, j)),
            scratch_shapes=[pltpu.VMEM((rows, count), BF16), pltpu.VMEM((rows, 1), F32)],
        ),
        out_shape=jax.ShapeDtypeStruct((rows, (last - first) * block), BF16),
        cost_estimate=cost(2 * rows * count * block * (last - first), 2 * block * (last - first) * (rows + count)),
        name="route",
    )(order, logit, ids, slot, keep, tokens)


def move(copies):
    for load, store in copies:
        load.start()
    for load, store in copies:
        load.wait()
        store.start()
    for load, store in copies:
        store.wait()


def pack_up_kernel(g_ref, u_ref, g_out, u_out, g_stage, u_stage, in_sem, out_sem):
    tall = g_out.shape[0]
    first = pl.multiple_of(lax.axis_index("dp") * tall, LANES)
    copies = []
    for i, (src, out, stage) in enumerate(((g_ref, g_out, g_stage), (u_ref, u_out, u_stage))):
        copies.append(
            (
                pltpu.make_async_copy(src.at[pl.ds(first, tall), :], stage, in_sem.at[i]),
                pltpu.make_async_copy(stage, out, out_sem.at[i]),
            )
        )
    move(copies)


def pack_up(gate, up_, planes):
    model, hidden = gate.shape
    shape = (model // planes, hidden)
    sems = pltpu.SemaphoreType.DMA((2,))
    return pl.pallas_call(
        pack_up_kernel,
        in_specs=[ANY] * 2,
        out_specs=[ANY] * 2,
        out_shape=[jax.ShapeDtypeStruct(shape, BF16)] * 2,
        scratch_shapes=[pltpu.VMEM(shape, BF16)] * 2 + [sems, sems],
        name="pack_up",
    )(gate, up_)


def pack_down_kernel(d_ref, out_ref, stage, in_sem, out_sem):
    tall, hidden = out_ref.shape
    first = lax.axis_index("dp") * tall
    copies = []
    for i in range(tall // hidden):
        span = slice(i * hidden, (i + 1) * hidden)
        copies.append(
            (
                pltpu.make_async_copy(columns(d_ref, first + i * hidden, hidden), stage.at[span, :], in_sem.at[i]),
                pltpu.make_async_copy(stage.at[span, :], out_ref.at[span, :], out_sem.at[i]),
            )
        )
    move(copies)


def pack_down(down_, planes):
    hidden, model = down_.shape
    shape = (model // planes, hidden)
    sems = pltpu.SemaphoreType.DMA((model // planes // hidden,))
    return pl.pallas_call(
        pack_down_kernel,
        in_specs=[ANY],
        out_specs=ANY,
        out_shape=jax.ShapeDtypeStruct(shape, BF16),
        scratch_shapes=[pltpu.VMEM(shape, BF16), sems, sems],
        name="pack_down",
    )(down_)


def by_slot(wide, value, sources, slots):
    tall, tiles = value.shape[0], value.shape[1] // LANES
    half = slots // 2
    for c in range(tiles):
        wide[c * tall : (c + 1) * tall, :] = value[:, c * LANES : (c + 1) * LANES].astype(F32)

    def group(first):
        return jnp.concatenate(
            [
                jnp.concatenate(
                    [wide[pl.ds(c * tall + s, sources, stride=slots), :].astype(BF16) for s in range(first, first + half)],
                    axis=0,
                )
                for c in range(tiles)
            ],
            axis=1,
        )

    return group(0), group(half)


class Staged:
    def __init__(self, groups, sems, ahead):
        self.groups = [[pltpu.make_async_copy(a, b, sems.at[n, i]) for i, (a, b) in enumerate(g)] for n, g in enumerate(groups)]
        self.ahead = ahead
        for n in range(ahead):
            self.begin(n)

    def begin(self, n):
        for copy in self.groups[n] if n < len(self.groups) else []:
            copy.start()

    def take(self, n):
        for copy in self.groups[n]:
            copy.wait()
        self.begin(n + self.ahead)


def up_pairs(order_ref, x_ref, x, tall_refs, side_refs, bufs, k, at, slot, cuts):
    width = x.shape[-1]
    part = width // cuts
    groups = []
    for c in range(cuts):
        inner = slice(c * part, (c + 1) * part)
        first = pl.multiple_of(order_ref[k] * width + c * part, LANES)
        pairs = [(x_ref.at[:, at * width + inner.start : at * width + inner.stop], x.at[slot, :, inner])]
        pairs += [(ref.at[pl.ds(first, part), :], buf.at[slot, inner, :]) for ref, buf in zip(tall_refs, bufs[:4])]
        pairs += [(ref.at[inner, :], buf.at[slot, inner, :]) for ref, buf in zip(side_refs, bufs[4:])]
        groups.append(pairs)
    return groups


def up_step(accs, x, bufs, wide, slot, c, cuts, fresh, sources, slots):
    part = x.shape[-1] // cuts
    inner = slice(c * part, (c + 1) * part)
    home, spill = by_slot(wide, x[slot, :, inner], sources, slots)
    hidden = bufs[0].shape[-1]
    for acc, rows, pair in zip(accs, (home, spill, spill), (bufs[0:2], bufs[2:4], bufs[4:6])):
        for i, buf in enumerate(pair):
            lanes = slice(i * hidden, (i + 1) * hidden)
            value = dot(rows, buf[slot, inner, :])
            acc[:, lanes] = value if fresh else acc[:, lanes] + value


def up_kernel(order_ref, x_ref, *refs, sources, slots, pieces):
    tall_refs, side_refs = refs[:4], refs[4 : 4 + 2 * pieces]
    out_ref, x, *bufs, wide, home_acc, near_acc, far_acc, sems, out_sem = refs[4 + 2 * pieces :]
    accs = (home_acc, near_acc, far_acc)
    groups = []
    for k in range(pieces):
        groups += up_pairs(order_ref, x_ref, x, tall_refs, (side_refs[k], side_refs[pieces + k]), bufs, k, k, k, CUTS)
    staged = Staged(groups, sems, AHEAD)
    for n in range(len(groups)):
        staged.take(n)
        up_step(accs, x, bufs, wide, n // CUTS, n % CUTS, CUTS, n == 0, sources, slots)
    stores = [pltpu.make_async_copy(acc, out_ref.at[i], out_sem.at[i]) for i, acc in enumerate(accs)]
    for copy in stores:
        copy.start()
    for copy in stores:
        copy.wait()


def up(order, x, own, partner, side_gate, side_up, sources, slots):
    rows = x.shape[0]
    hidden = own[0].shape[-1]
    pieces = len(side_gate)
    part = x.shape[1] // pieces
    acc = pltpu.VMEM((rows // 2, 2 * hidden), F32)
    return pl.pallas_call(
        functools.partial(up_kernel, sources=sources, slots=slots, pieces=pieces),
        in_specs=[SCALARS] + [ANY] * (5 + 2 * pieces),
        out_specs=ANY,
        out_shape=jax.ShapeDtypeStruct((3, rows // 2, 2 * hidden), F32),
        scratch_shapes=[pltpu.VMEM((pieces, rows, part), BF16)]
        + [pltpu.VMEM((pieces, part, hidden), BF16)] * 6
        + [pltpu.VMEM((rows * part // CUTS // LANES, LANES), F32), acc, acc, acc]
        + [pltpu.SemaphoreType.DMA((pieces * CUTS, 7)), pltpu.SemaphoreType.DMA((3,))],
        cost_estimate=cost(6 * rows * x.shape[1] * hidden, 2 * x.shape[1] * (rows + 6 * hidden)),
        name="up",
    )(order, x, own[0], own[1], partner[0], partner[1], *side_gate, *side_up)


def ffn_kernel(flag_ref, order_ref, x_ref, sum_ref, *refs, sources, slots, planes):
    tall_refs, side_refs, (d0_ref, d1_ref), side_down = refs[:4], refs[4:6], refs[6:8], refs[8 : 8 + planes + 1]
    out_ref, x, *bufs, d0, d1, d2, sums, out, wide, tail, hid, sems, out_sem = refs[8 + planes + 1 :]
    width = x.shape[-1]
    tall = x.shape[1]
    hidden = bufs[0].shape[-1]
    half = slots // 2
    rows = sources * half
    last = planes - 1
    groups = up_pairs(order_ref, x_ref, x, tall_refs, side_refs, bufs, last, 0, 0, CUTS)
    groups[0].append((sum_ref, sums))
    stores = []
    for k in range(planes):
        first = order_ref[k] * width
        pairs = [(columns(d0_ref, first, width), d0.at[k]), (columns(d1_ref, first, width), d1.at[k])]
        if k < last:
            pairs.append((side_down[k], d2.at[k]))
        else:
            pairs.append((side_down[last], d2.at[k, 0 : width // 2, :]))
            pairs.append((side_down[last + 1], d2.at[k, width // 2 : width, :]))
        groups.append(pairs)
        stores.append(pltpu.make_async_copy(out.at[k], columns(out_ref, first, width), out_sem.at[k]))
    staged = Staged(groups, sems, AHEAD)
    accs = [sums.at[i] for i in range(3)]
    for c in range(CUTS):
        staged.take(c)
        up_step(accs, x, bufs, wide, 0, c, CUTS, False, sources, slots)

    def activate(acc):
        gate = acc[:, 0:hidden]
        return (gate / (1.0 + jnp.exp(-gate)) * acc[:, hidden : 2 * hidden]).astype(BF16)

    hid[0:rows, :] = activate(sums[0])
    for j in range(half):
        cut = slice(j * sources, (j + 1) * sources)
        use_near = flag_ref[j] == 1
        mine = activate(jnp.where(use_near, sums[1, cut, :], sums[2, cut, :])).astype(F32)
        hid[rows + cut.start : rows + cut.stop, :] = jnp.where(use_near, mine, 0.0).astype(BF16)
        hid[2 * rows + cut.start : 2 * rows + cut.stop, :] = jnp.where(use_near, 0.0, mine).astype(BF16)

    for k in range(planes):
        staged.take(CUTS + k)
        home = dot(hid[0:rows, :], d0[k])
        far = jnp.concatenate(
            [dot(hid[2 * rows :, :], d2[k, i * hidden : (i + 1) * hidden, :]) for i in range(width // hidden)], axis=1
        )
        spill = dot(hid[rows : 2 * rows, :], d1[k]) + far
        for c in range(width // LANES):
            lanes = slice(c * LANES, (c + 1) * LANES)
            for s in range(half):
                cut = slice(s * sources, (s + 1) * sources)
                tail[pl.ds(c * tall + s, sources, stride=slots), :] = home[cut, lanes]
                tail[pl.ds(c * tall + half + s, sources, stride=slots), :] = spill[cut, lanes]
            out[k, :, lanes] = tail[c * tall : (c + 1) * tall, :].astype(BF16)
        stores[k].start()
    for copy in stores:
        copy.wait()


def ffn(flags, order, x, sums, own, partner, side_gate, side_up, side_down, sources, slots, planes):
    rows, width = x.shape
    hidden = own[0].shape[-1]
    model = width * planes
    flat = pltpu.VMEM((planes, hidden, width), BF16)
    return call(
        functools.partial(ffn_kernel, sources=sources, slots=slots, planes=planes),
        (rows, model),
        [SCALARS] * 2 + [ANY] * (10 + len(side_down)),
        [pltpu.VMEM((1, rows, width), BF16)]
        + [pltpu.VMEM((1, width, hidden), BF16)] * 6
        + [flat, flat, pltpu.VMEM((planes, width, hidden), BF16), pltpu.VMEM(sums.shape, F32)]
        + [pltpu.VMEM((planes, rows, width), BF16), pltpu.VMEM((rows * width // CUTS // LANES, LANES), F32)]
        + [pltpu.VMEM((rows * width // LANES, LANES), F32), pltpu.VMEM((3 * rows // 2, hidden), BF16)]
        + [pltpu.SemaphoreType.DMA((CUTS + planes, 8)), pltpu.SemaphoreType.DMA((planes,))],
        2 * rows * model * hidden,
        2 * model * (rows + 3 * hidden),
    )(flags, order, x, sums, own[0], own[1], partner[0], partner[1], side_gate, side_up, own[2], partner[2], *side_down)


def finish_kernel(cell_ref, sh_ref, sd_ref, ans_ref, out_ref, chosen):
    @pl.when(pl.program_id(0) == 0)
    def _():
        hit = lax.broadcasted_iota(jnp.int32, chosen.shape, 1) == cell_ref[...]
        chosen[...] = hit.astype(F32).astype(BF16)

    out = dot(chosen[...], ans_ref[...]) + dot(sh_ref[...], sd_ref[...])
    out_ref[...] = out.astype(BF16)


def finish(cell, sh, sd, answers, parts=2):
    count = cell.shape[0]
    rows, width = answers.shape
    block = width // parts
    return pl.pallas_call(
        finish_kernel,
        grid=(parts,),
        in_specs=[
            pl.BlockSpec((count, 1), lambda j: (0, 0)),
            pl.BlockSpec(sh.shape, lambda j: (0, 0)),
            pl.BlockSpec((sd.shape[0], block), lambda j: (0, j)),
            pl.BlockSpec((rows, block), lambda j: (0, j)),
        ],
        out_specs=pl.BlockSpec((count, block), lambda j: (0, j)),
        out_shape=jax.ShapeDtypeStruct((count, width), BF16),
        scratch_shapes=[pltpu.VMEM((count, rows), BF16)],
        cost_estimate=cost(2 * rows * count * width, 2 * width * (rows + 2 * count)),
        name="finish",
    )(cell, sh, sd, answers)


def exchange(x, experts):
    rows, width = x.shape
    x = x.reshape(experts, rows // experts, width)
    x = lax.all_to_all(x, "expert", split_axis=0, concat_axis=0, tiled=True)
    return x.reshape(rows, width)


def ring(planes, step):
    return [(p, (p + step) % planes) for p in range(planes)]


def nearest(piece, planes):
    return [piece, lax.ppermute(piece, "dp", ring(planes, 1)), lax.ppermute(piece, "dp", ring(planes, -1))]


def body(
    tokens,
    router_logit,
    expert_id,
    token_slot,
    keep,
    overflow_host,
    expert_gate,
    expert_up,
    expert_down,
    shared_gate,
    shared_up,
    shared_down,
):
    experts = lax.axis_size("expert")
    planes = lax.axis_size("dp")
    myself = lax.axis_index("expert")
    count, model = tokens.shape
    slots = 2 * count // experts
    rows = experts * slots
    gate, up_, down_ = expert_gate[0], expert_up[0], expert_down[0]
    plane = lax.axis_index("dp")
    order = (plane + jnp.array([0, planes - 1, 1, 2], jnp.int32)) % planes
    side_pairs = [(e, (e + 1 if e % 2 else e - 1) % experts) for e in range(experts)]
    partner_pairs = [(e, e ^ 1) for e in range(experts)]
    block = model // planes
    gate_part, up_part = [lax.ppermute(w, "expert", side_pairs) for w in pack_up(gate, up_, planes)]

    line = lambda v: v.reshape(1, count)
    routing = (order, line(router_logit), line(expert_id), line(token_slot), line(keep), tokens, rows, slots, block)
    outgoing = route(*routing, 0, planes - 1)
    arrived = exchange(outgoing, experts)
    outgoing = route(*routing, planes - 1, planes)

    side_gate, side_up = nearest(gate_part, planes), nearest(up_part, planes)
    far_gate = lax.ppermute(side_gate[1], "dp", ring(planes, 1))
    far_up = lax.ppermute(side_up[2], "dp", ring(planes, -1))
    gate1, up1, down1 = [lax.ppermute(w, "expert", partner_pairs) for w in (gate, up_, down_)]
    host_row = lax.dynamic_index_in_dim(overflow_host, myself, 0, keepdims=False)
    flags = (host_row == (myself ^ 1)).astype(jnp.int32)

    down_part, side_gate, side_up, far_gate, far_up = lax.optimization_barrier(
        (pack_down(down_, planes), side_gate, side_up, far_gate, far_up)
    )
    down_part = lax.ppermute(down_part, "expert", side_pairs)
    arrived2 = exchange(outgoing, experts)
    side_down = nearest(down_part, planes)
    half = block // 2
    side_down.append(lax.ppermute(side_down[1][:half], "dp", ring(planes, 1)))
    side_down.append(lax.ppermute(side_down[2][half:], "dp", ring(planes, -1)))

    sums = up(order, arrived, (gate, up_), (gate1, up1), side_gate, side_up, experts, slots)
    reply = ffn(
        flags, order, arrived2, sums, (gate, up_, down_), (gate1, up1, down1), far_gate, far_up, side_down, experts, slots, planes
    )
    answers = exchange(reply, experts)
    shared_hidden = (
        jax.nn.silu(jnp.dot(tokens, shared_gate, preferred_element_type=F32))
        * jnp.dot(tokens, shared_up, preferred_element_type=F32)
    ).astype(BF16)
    cell = (expert_id * slots + token_slot).reshape(count, 1)
    return finish(cell, shared_hidden, shared_down, answers)


def solution(mesh):
    return jax.shard_map(
        body,
        mesh=mesh,
        in_specs=(
            P(("dp", "expert"), None),
            P(("dp", "expert")),
            P(("dp", "expert")),
            P(("dp", "expert")),
            P(("dp", "expert")),
            P(),
            P("expert", None, None),
            P("expert", None, None),
            P("expert", None, None),
            P(),
            P(),
            P(),
        ),
        out_specs=P(("dp", "expert"), None),
        check_vma=False,
    )
```
